32 devices in a mesh: aa: 8 (over z, x), ba: 4 (over y, core).
Axes of the slice: x: 2, y: 2, z: 4, core: 2. Of those that a mesh axis runs over, the one named last changes fastest.
Arguments:
- grid_features: bfloat16 [128, 128, 256, 128], P('aa', 'ba'), may hold values from -6 to 6
- weight_real: bfloat16 [32, 32, 16, 128, 128], P('ba', None, 'aa'), may hold values from -6 to 6
- weight_imag: bfloat16 [32, 32, 16, 128, 128], P('ba', None, 'aa'), may hold values from -6 to 6
- mode_keep: int32 [32, 16], P('ba', 'aa'), may hold values from 1 to 16, as said below
- local_weight: bfloat16 [128, 128], replicated, may hold values from -0.5 to 0.5
- local_bias: bfloat16 [128], replicated, may hold values from -3 to 3
Outputs:
- layer_output: bfloat16 [128, 128, 256, 128], P('aa', 'ba')
The draws below stay inside these ranges and needn't reach their ends.
Inputs may be any that keep to these rules, and one draw needn't show every extreme that they name: mode_keep[i, k] counts the retained levels of the second frequency on the line of the i-th retained first frequency and the k-th third frequency.
All inputs are finite; a program needn't handle non-finite values.
Results may differ from the reference program's by a relative error of at most 0.012.
Values may be sent and summed in bfloat16 or wider, within the bound.
No kernel may reach another device: no remote copies, remote signals or barrier semaphores. Data moves between devices by JAX's collectives and lax.ppermute only.
A program may use at most 256 MiB of HBM per device.

```python
import math
import jax
import jax.numpy as jnp
from jax import lax

NX = 128
NY = 128
NZ = 256
C = 128
KX = 32
KY = 32
KZ = 16
N_AA = 8


def draw_mode_keep(key, part):
    top_level = KY // 2
    positions = jnp.arange(KX, dtype=jnp.int32)
    level_first = jnp.where(positions < KX // 2, positions, KX - 1 - positions)
    level_third = jnp.arange(KZ, dtype=jnp.int32)
    reach_total = KX // 2 + KZ
    base_level = top_level - (level_first[:, None] + level_third[None, :]) * top_level // reach_total
    jitter = jax.random.randint(key, (KX, KZ), -3, 4, dtype=jnp.int32)
    kept_levels = jnp.clip(base_level + jitter, 1, top_level)
    kept_levels = kept_levels.at[0, 0].set(top_level)
    kept_levels = kept_levels.at[KX // 2 - 1, KZ - 1].set(1)
    return kept_levels.astype(jnp.int32)


def block_levels(own_key, dims, shards, low, top_value):
    def one(dim, shards_of):
        draws = jax.random.uniform(jax.random.fold_in(jax.random.fold_in(own_key, 6), dim), (shards_of,), jnp.float32, low / len(shards), top_value / len(shards))
        return jnp.repeat(jnp.exp(draws), dims[dim] // shards_of).reshape((-1,) + (1,) * (len(dims) - dim - 1))

    gain = one(*shards[0])
    for cut in shards[1:]:
        gain = gain * one(*cut)
    return gain


def centred(rng, extent, spread, limit, pieces=(), kind=jnp.bfloat16):
    drawn = jax.random.normal(rng, extent, jnp.float32) * spread
    if len(pieces) > 0:
        drawn = block_levels(rng, extent, pieces, -0.22, 0.18) * drawn
    return jnp.clip(drawn, min=-limit, max=limit).astype(kind)


def setup_inputs(seed: int = 0) -> dict:
    keys = jax.random.split(jax.random.key(seed), 7)
    grid_features = centred(keys[0], (NX, NY, NZ, C), 1.0, 6.0, ((0, 8), (1, 4)))
    weight_real = centred(keys[1], (KX, KY, KZ, C, C), 1.0, 6.0, ((0, 4), (2, 8)))
    weight_imag = centred(keys[2], (KX, KY, KZ, C, C), 1.0, 6.0, ((0, 4), (2, 8)))
    mode_keep = draw_mode_keep(jax.random.fold_in(keys[6], 71), 0)
    local_weight = centred(keys[4], (C, C), C ** -0.5, 0.5)
    local_bias = centred(keys[5], (C,), 0.5, 3.0)
    return {"grid_features": grid_features, "weight_real": weight_real, "weight_imag": weight_imag, "mode_keep": mode_keep, "local_weight": local_weight, "local_bias": local_bias}


highest = lax.Precision.HIGHEST


def kept_modes(length, number):
    positions = jnp.arange(number, dtype=jnp.int32)
    return jnp.where(positions < number // 2, positions, positions + (length - number)).astype(jnp.int32)


def phase_tables(length, mode_list):
    places = jnp.arange(length, dtype=jnp.int32)
    phase_steps = (places[:, None] * mode_list[None, :]) % length
    angles = phase_steps.astype(jnp.float32) * (2.0 * math.pi / length)
    return jnp.cos(angles), jnp.sin(angles)


def forward_kernel(length, number):
    cosine_table, sine_table = phase_tables(length, kept_modes(length, number))
    upper_rows = jnp.concatenate([cosine_table, -sine_table], axis=1)
    lower_rows = jnp.concatenate([sine_table, cosine_table], axis=1)
    return jnp.concatenate([upper_rows, lower_rows], axis=0)


def inverse_kernel(length, number):
    cosine_table, sine_table = phase_tables(length, kept_modes(length, number))
    upper_rows = jnp.concatenate([cosine_table.T, sine_table.T], axis=1)
    lower_rows = jnp.concatenate([-sine_table.T, cosine_table.T], axis=1)
    return jnp.concatenate([upper_rows, lower_rows], axis=0)


def depth_kernels():
    cosine_table, sine_table = phase_tables(NZ, jnp.arange(KZ, dtype=jnp.int32))
    forward = jnp.concatenate([cosine_table, -sine_table], axis=1).astype(jnp.bfloat16)
    factor = jnp.where(jnp.arange(KZ, dtype=jnp.int32) == 0, 1.0, 2.0).astype(jnp.float32) / (NX * NY * NZ)
    inverse = jnp.concatenate([cosine_table.T * factor[:, None], -sine_table.T * factor[:, None]], axis=0).astype(jnp.bfloat16)
    return forward, inverse


def along_first(operand, kernel):
    return jnp.einsum('pabc,pq->qabc', operand, kernel, precision=highest, preferred_element_type=jnp.float32)


def along_second(operand, kernel):
    return jnp.einsum('apbc,pq->aqbc', operand, kernel, precision=highest, preferred_element_type=jnp.float32)


def mode_mask(kept_counts):
    positions = jnp.arange(KY, dtype=jnp.int32)
    levels = jnp.where(positions < KY // 2, positions, KY - 1 - positions)
    return (levels[None, :, None] < kept_counts[:, None, :]).astype(jnp.float32)


def reference(grid_features, weight_real, weight_imag, mode_keep, local_weight, local_bias):
    forward_depth, inverse_depth = depth_kernels()
    slab_rows = NX // N_AA
    field_slabs = grid_features.reshape(N_AA, slab_rows, NY, NZ, C)

    def depth_forward(slab_cells):
        flat_rows = jnp.transpose(slab_cells, (0, 1, 3, 2)).reshape(slab_rows * NY * C, NZ).astype(jnp.float32)
        coeffs = jnp.dot(flat_rows, forward_depth.astype(jnp.float32), precision=highest, preferred_element_type=jnp.float32)
        coeffs = jnp.transpose(coeffs.reshape(slab_rows, NY, C, 2 * KZ), (0, 1, 3, 2))
        return coeffs.astype(jnp.bfloat16)

    coeffs = lax.map(depth_forward, field_slabs).reshape(NX, NY, 2 * KZ, C)
    stacked = jnp.concatenate([coeffs[:, :, :KZ], coeffs[:, :, KZ:]], axis=0).astype(jnp.float32)
    result = along_first(stacked, forward_kernel(NX, KX))
    result = jnp.concatenate([result[:KX], result[KX:]], axis=1)
    result = along_second(result, forward_kernel(NY, KY)).astype(jnp.bfloat16)
    spec_real = result[:, :KY]
    spec_imag = result[:, KY:]

    def mix_line(operands):
        real_part, imag_part, line_real, line_imag = operands
        real_part = real_part.astype(jnp.float32)
        imag_part = imag_part.astype(jnp.float32)
        line_real = line_real.astype(jnp.float32)
        line_imag = line_imag.astype(jnp.float32)
        pattern = 'bcd,bcde->bce'
        out_real = jnp.einsum(pattern, real_part, line_real, precision=highest) - jnp.einsum(pattern, imag_part, line_imag, precision=highest)
        out_imag = jnp.einsum(pattern, real_part, line_imag, precision=highest) + jnp.einsum(pattern, imag_part, line_real, precision=highest)
        return out_real, out_imag

    mixed_real, mixed_imag = lax.map(mix_line, (spec_real, spec_imag, weight_real, weight_imag))
    keep_mask = mode_mask(mode_keep)[..., None]
    mixed_real = mixed_real * keep_mask
    mixed_imag = mixed_imag * keep_mask
    result = along_second(jnp.concatenate([mixed_real, mixed_imag], axis=1), inverse_kernel(NY, KY))
    result = jnp.concatenate([result[:, :NY], result[:, NY:]], axis=0)
    result = along_first(result, inverse_kernel(NX, KX)).astype(jnp.bfloat16)
    back_field = jnp.concatenate([result[:NX], result[NX:]], axis=2)
    back_slabs = back_field.reshape(N_AA, slab_rows, NY, 2 * KZ, C)

    def finish_slab(operands):
        slab_cells, back_slab = operands
        flat_rows = jnp.transpose(back_slab, (0, 1, 3, 2)).reshape(slab_rows * NY * C, 2 * KZ).astype(jnp.float32)
        spectral = jnp.dot(flat_rows, inverse_depth.astype(jnp.float32), precision=highest, preferred_element_type=jnp.float32)
        spectral = jnp.transpose(spectral.reshape(slab_rows, NY, C, NZ), (0, 1, 3, 2))
        local_term = jnp.dot(slab_cells.reshape(-1, C).astype(jnp.float32), local_weight.astype(jnp.float32), precision=highest, preferred_element_type=jnp.float32)
        local_term = local_term.reshape(slab_rows, NY, NZ, C)
        return jax.nn.gelu(spectral + local_term + local_bias.astype(jnp.float32)).astype(jnp.bfloat16)

    return lax.map(finish_slab, (field_slabs, back_slabs)).reshape(NX, NY, NZ, C)
```

```python
import jax
import jax.numpy as jnp
import numpy as np
from jax import lax
from jax.experimental import pallas as pl
from jax.experimental.pallas import tpu as pltpu
from jax.sharding import PartitionSpec as P

BF = jnp.bfloat16
F32 = jnp.float32
CHUNKS = 2


def kept_modes(length, number):
    pos = np.arange(number)
    return np.where(pos < number // 2, pos, pos + (length - number))


def tables(length, modes):
    steps = (np.arange(length)[:, None] * modes[None, :]) % length
    angles = steps.astype(np.float64) * (2.0 * np.pi / length)
    return np.cos(angles), np.sin(angles)


def block_order(count):
    order = [0]
    bit = count // 2
    while bit:
        order = order + [q + bit for q in order]
        bit //= 2
    return order


def dot(a, b):
    return jnp.dot(a, b, preferred_element_type=F32)


def swap(x, count, bit):
    return lax.ppermute(x, "ba", [(i, i ^ bit) for i in range(count)])


def forward_plane(g, fz, ty, chunk, chunks, na, nb, kz2, kyl):
    Xl, Yl, NZ, C = g.shape
    KZ = kz2 * na
    Xc = Xl // chunks
    half = nb // 2
    rows = 2 * kyl

    def body(g_ref, fz_ref, ty_ref, rest_ref, send_ref, s_ref):
        fzv = fz_ref[...]
        for y in range(0, Yl, 2):
            r = dot(fzv, jnp.concatenate([g_ref[0, y], g_ref[0, y + 1]], axis=1))
            s_ref[pl.ds(y, 2 * KZ, stride=Yl), :] = r[:, :C]
            s_ref[pl.ds(y + 1, 2 * KZ, stride=Yl), :] = r[:, C:]
        tyv = ty_ref[...]
        for k in range(0, KZ, 2):
            lo = s_ref[k * 2 * Yl : (k + 1) * 2 * Yl, :]
            hi = s_ref[(k + 1) * 2 * Yl : (k + 2) * 2 * Yl, :]
            o = dot(tyv, jnp.concatenate([lo, hi], axis=1).astype(BF)).astype(BF)
            for u in range(2):
                a, j = divmod(k + u, kz2)
                for n in range(nb):
                    ref = rest_ref if n < half else send_ref
                    ref[n % half, a, 0, j] = o[n * rows : (n + 1) * rows, u * C : (u + 1) * C]

    shape = (half, na, Xc, kz2, rows, C)
    block = pl.BlockSpec((half, na, 1, kz2, rows, C), lambda x: (0, 0, x, 0, 0, 0))
    out = jax.ShapeDtypeStruct(shape, BF)
    return pl.pallas_call(
        body,
        grid=(Xc,),
        in_specs=[
            pl.BlockSpec((1, Yl, NZ, C), lambda x: (x + chunk * Xc, 0, 0, 0)),
            pl.BlockSpec(fz.shape, lambda x: (0, 0)),
            pl.BlockSpec(ty.shape, lambda x: (0, 0)),
        ],
        out_specs=[block, block],
        out_shape=[out, out],
        scratch_shapes=[pltpu.VMEM((2 * KZ * Yl, C), F32)],
        name="forward_plane",
    )(g, fz, ty)


def forward_first(parts, tx, nb, kxl, kz2, kyl, C):
    KX = kxl * nb
    NX = tx.shape[1] // 2
    R = kz2 * 2 * kyl
    count = len(parts)

    def body(*refs):
        tx_ref = refs[count]
        o_ref, s_ref = refs[count + 1 :]
        size = NX * R // count
        for h in range(count):
            s_ref[h * size : (h + 1) * size, :] = refs[h][...].astype(F32)
        txv = tx_ref[...]
        for j in range(kz2):
            cols = []
            for m in range(kyl):
                parts_ = [
                    s_ref[pl.ds(j * 2 * kyl + ri * kyl + m, NX, stride=R), :] for ri in range(2)
                ]
                cols.append(jnp.concatenate(parts_, axis=0).astype(BF))
            o = dot(txv, jnp.concatenate(cols, axis=1)).astype(BF)
            for n in range(nb):
                for m in range(kyl):
                    o_ref[n, j, m] = o[
                        n * 2 * kxl : (n + 1) * 2 * kxl, m * C : (m + 1) * C
                    ]

    return pl.pallas_call(
        body,
        out_shape=jax.ShapeDtypeStruct((nb, kz2, kyl, 2 * kxl, C), BF),
        scratch_shapes=[pltpu.VMEM((NX * R, C), F32)],
        name="forward_first",
    )(*[p.reshape(-1, C) for p in parts], tx)


def mix(spec, wr, wi, keep):
    nb, kz2, kyl, rows, C = spec.shape
    kxl, KY = wr.shape[:2]
    kyc = min(4, kyl)
    steps = kyl // kyc
    levels = jnp.broadcast_to(keep.T[:, :, None], (kz2, kxl, C))

    def body(s_ref, wr_ref, wi_ref, keep_ref, o_ref):
        base = pl.program_id(1) * kyc
        row = lax.broadcasted_iota(jnp.int32, (rows, 2 * C), 0)
        row = jnp.where(row >= kxl, row - kxl, row)
        kept = keep_ref[0]
        for t in range(kyc):
            ky = base + t
            level = jnp.where(ky < KY // 2, ky, KY - 1 - ky)
            s = s_ref[0, 0, t]
            acc = None
            for i in range(kxl):
                w = jnp.concatenate([wr_ref[i, t, 0], wi_ref[i, t, 0]], axis=1)
                res = dot(s, w)
                acc = res if acc is None else jnp.where(row == i, res, acc)
            re = acc[:kxl, :C] - acc[kxl:, C:]
            im = acc[:kxl, C:] + acc[kxl:, :C]
            on = level < kept
            re = jnp.where(on, re, 0.0)
            im = jnp.where(on, im, 0.0)
            o_ref[0, 0, t] = jnp.concatenate([re, im], axis=0).astype(BF)

    sblock = pl.BlockSpec((1, 1, kyc, rows, C), lambda j, s: (s // steps, j, s % steps, 0, 0))
    wblock = pl.BlockSpec((kxl, kyc, 1, C, C), lambda j, s: (0, s, j, 0, 0))
    return pl.pallas_call(
        body,
        grid=(kz2, nb * steps),
        in_specs=[sblock, wblock, wblock, pl.BlockSpec((1, kxl, C), lambda j, s: (j, 0, 0))],
        out_specs=sblock,
        out_shape=jax.ShapeDtypeStruct(spec.shape, BF),
        name="mix",
    )(spec, wr, wi, levels)


def inverse_first(mixed, txi, chunks, na):
    nb, kz2, kyl, rows, C = mixed.shape
    NX = txi.shape[0] // 2
    R = kz2 * 2 * kyl
    size = NX * R // chunks

    def body(m_ref, tx_ref, *rest):
        outs, s_ref = rest[:chunks], rest[chunks]
        txv = tx_ref[...]
        for j in range(kz2):
            cols = [
                jnp.concatenate([m_ref[n, j, m] for n in range(nb)], axis=0) for m in range(kyl)
            ]
            o = dot(txv, jnp.concatenate(cols, axis=1))
            for ri in range(2):
                for m in range(kyl):
                    s_ref[pl.ds(j * 2 * kyl + ri * kyl + m, NX, stride=R), :] = o[
                        ri * NX : (ri + 1) * NX, m * C : (m + 1) * C
                    ]
        for h in range(chunks):
            outs[h][...] = s_ref[h * size : (h + 1) * size, :].astype(BF)

    outs = pl.pallas_call(
        body,
        out_shape=[jax.ShapeDtypeStruct((size, C), BF)] * chunks,
        scratch_shapes=[pltpu.VMEM((NX * R, C), F32)],
        name="inverse_first",
    )(mixed, txi)
    Xc = NX // na // chunks
    return [o.reshape(na, Xc, kz2, 2 * kyl, C) for o in outs]


def finish(g, pieces, uy, iz, lw2, lb2, prior, chunk, chunks):
    Xl, Yl, NZ, C = g.shape
    na, Xc, kz2, rows, _ = pieces[0].shape
    KZ = na * kz2
    nb = len(pieces)

    def body(*refs):
        g_ref, uy_ref, iz_ref, lw_ref, lb_ref = refs[:5]
        p_refs = refs[5 : 5 + nb]
        o_ref, s_ref = refs[-2:]
        uyv = uy_ref[...]
        for k in range(0, KZ, 2):
            cols = []
            for u in range(2):
                a, j = divmod(k + u, kz2)
                cols.append(jnp.concatenate([p[a, 0, j] for p in p_refs], axis=0))
            o = dot(uyv, jnp.concatenate(cols, axis=1))
            for u in range(2):
                for ri in range(2):
                    s_ref[pl.ds((k + u) * 2 + ri, Yl, stride=2 * KZ), :] = o[
                        ri * Yl : (ri + 1) * Yl, u * C : (u + 1) * C
                    ]

        lwv = lw_ref[...]
        izv = iz_ref[...]
        lbv = lb_ref[...]

        def step(t, carry):
            y = t * 2
            lo = s_ref[pl.ds(pl.multiple_of(y * 2 * KZ, 2 * KZ), 2 * KZ), :]
            hi = s_ref[pl.ds(pl.multiple_of((y + 1) * 2 * KZ, 2 * KZ), 2 * KZ), :]
            b = jnp.concatenate([lo, hi], axis=1).astype(BF)
            cells = jnp.concatenate([g_ref[0, y], g_ref[0, y + 1], izv], axis=1)
            maps = jnp.concatenate([lwv, b, lbv], axis=0)
            v = dot(cells, maps).astype(BF)
            inner = v * (BF(0.7978845608028654) + BF(0.035677408136300125) * (v * v))
            half = BF(0.5) * v
            r = half + half * jnp.tanh(inner)
            o_ref[0, y] = r[:, :C]
            o_ref[0, y + 1] = r[:, C:]
            return carry

        lax.fori_loop(0, Yl // 2, step, 0, unroll=4)

    whole = lambda a: pl.BlockSpec(a.shape, lambda x: (0,) * a.ndim)
    cell = pl.BlockSpec((1, Yl, NZ, C), lambda x: (x + chunk * Xc, 0, 0, 0))
    piece = pl.BlockSpec((na, 1, kz2, rows, C), lambda x: (0, x, 0, 0, 0))
    args = [g, uy, iz, lw2, lb2, *pieces]
    specs = [cell, whole(uy), whole(iz), whole(lw2), whole(lb2)] + [piece] * nb
    aliases = {}
    if prior is not None:
        aliases = {len(args): 0}
        args.append(prior)
        specs.append(pl.BlockSpec(memory_space=pl.ANY))
    return pl.pallas_call(
        body,
        grid=(Xc,),
        in_specs=specs,
        out_specs=cell,
        out_shape=jax.ShapeDtypeStruct(g.shape, BF),
        scratch_shapes=[pltpu.VMEM((2 * KZ * Yl, C), F32)],
        input_output_aliases=aliases,
        name="finish",
    )(*args)


def stack_forward(cos, sin):
    return np.block([[cos.T, sin.T], [-sin.T, cos.T]])


def solution(mesh):
    na, nb = mesh.shape["aa"], mesh.shape["ba"]

    def per_device(g, wr, wi, keep, lw, lb):
        Xl, Yl, NZ, C = g.shape
        kxl, KY, kz2 = wr.shape[:3]
        NX, NY, KX, KZ, kyl = Xl * na, Yl * nb, kxl * nb, kz2 * na, KY // nb
        chunks = CHUNKS
        Xc = Xl // chunks
        order = block_order(nb)

        cz, sz = tables(NZ, np.arange(KZ))
        fz = np.stack([cz.T, -sz.T], axis=1).reshape(2 * KZ, NZ).astype(BF)
        factor = np.where(np.arange(KZ) == 0, 1.0, 2.0) / (NX * NY * NZ)
        iz = np.stack([cz * factor, -sz * factor], axis=2).reshape(NZ, 2 * KZ).astype(BF)

        cy, sy = tables(NY, kept_modes(NY, KY))
        ty_all, uy_all = [], []
        for b in range(nb):
            rows = slice(b * Yl, (b + 1) * Yl)
            ty, uy = [], []
            for q in order:
                cols = slice((b ^ q) * kyl, ((b ^ q) + 1) * kyl)
                c, s = cy[rows, cols], sy[rows, cols]
                ty.append(np.block([[c.T, s.T], [-s.T, c.T]]))
                uy.append(np.block([[c, -s], [s, c]]))
            ty_all.append(np.concatenate(ty, axis=0))
            uy_all.append(np.concatenate(uy, axis=1))
        me = lax.axis_index("ba")
        ty = lax.dynamic_index_in_dim(jnp.asarray(np.stack(ty_all).astype(BF)), me, 0, False)
        uy = lax.dynamic_index_in_dim(jnp.asarray(np.stack(uy_all).astype(BF)), me, 0, False)

        cx, sx = tables(NX, kept_modes(NX, KX))
        places = np.arange(NX).reshape(na, chunks, Xc).transpose(1, 0, 2).reshape(-1)
        cx, sx = cx[places], sx[places]
        tx, txi = [], []
        for n in range(nb):
            c, s = cx[:, n * kxl : (n + 1) * kxl], sx[:, n * kxl : (n + 1) * kxl]
            tx.append(np.block([[c.T, s.T], [-s.T, c.T]]))
            txi.append(np.block([[c, -s], [s, c]]))
        tx = jnp.asarray(np.concatenate(tx, axis=0).astype(BF))
        txi = jnp.asarray(np.concatenate(txi, axis=1).astype(BF))

        parts = []
        for h in range(chunks):
            rest, send = forward_plane(g, jnp.asarray(fz), ty, h, chunks, na, nb, kz2, kyl)
            bit = 1
            while True:
                got = swap(send, nb, bit)
                rest = (rest.astype(F32) + got.astype(F32)).astype(BF)
                bit *= 2
                if bit == nb:
                    break
                mid = rest.shape[0] // 2
                rest, send = rest[:mid], rest[mid:]
            parts.append(lax.all_to_all(rest[0], "aa", 0, 0, tiled=True))
        spec = forward_first(parts, tx, nb, kxl, kz2, kyl, C)
        spec = lax.all_to_all(spec, "ba", 0, 0, tiled=True)
        mixed = mix(spec, wr, wi, keep)
        mixed = lax.all_to_all(mixed, "ba", 0, 0, tiled=True)
        backs = inverse_first(mixed, txi, chunks, na)

        zero = jnp.zeros_like(lw)
        lw2 = jnp.concatenate(
            [jnp.concatenate([lw, zero], axis=1), jnp.concatenate([zero, lw], axis=1)], axis=0
        )
        lb2 = jnp.pad(jnp.tile(lb, 2)[None, :], ((0, 15), (0, 0)))
        iz = np.concatenate([iz, np.ones((NZ, 1)), np.zeros((NZ, 15))], axis=1).astype(BF)
        out = None
        for h in range(chunks):
            pieces = [lax.all_to_all(backs[h], "aa", 0, 0, tiled=True)]
            bit = nb // 2
            while bit:
                pieces = pieces + [swap(p, nb, bit) for p in pieces]
                bit //= 2
            out = finish(g, pieces, uy, jnp.asarray(iz), lw2, lb2, out, h, chunks)
        return out

    in_specs = (
        P("aa", "ba", None, None),
        P("ba", None, "aa", None, None),
        P("ba", None, "aa", None, None),
        P("ba", "aa"),
        P(),
        P(),
    )
    return jax.shard_map(
        per_device,
        mesh=mesh,
        in_specs=in_specs,
        out_specs=P("aa", "ba", None, None),
        check_vma=False,
    )
```
